32 devices in a mesh: dp: 4 (over x, core), tensor: 4 (over z), section: 2 (over y).
Axes of the slice: x: 2, y: 2, z: 4, core: 2. Of those that a mesh axis runs over, the one named last changes fastest.
Arguments:
- patches: bfloat16 [16, 256, 1152], P(('dp', 'section'), 'tensor'), may hold values from -6 to 6
- teacher: int32 [16, 7], P(('dp', 'section')), may hold values from 0 to 255
- proj_w: bfloat16 [1152, 4096], P(None, ('dp', 'tensor', 'section')), may hold values from -0.1875 to 0.1875
- norm_gain: bfloat16 [4096], replicated, may hold values from 0.25 to 1.75
- wq: bfloat16 [4096, 4096], P(('dp', 'section'), 'tensor'), may hold values from -0.09375 to 0.09375
- wk: bfloat16 [4096, 4096], P(('dp', 'section'), 'tensor'), may hold values from -0.09375 to 0.09375
- wv: bfloat16 [4096, 4096], P(('dp', 'section'), 'tensor'), may hold values from -0.09375 to 0.09375
- wo: bfloat16 [4096, 4096], P('tensor', ('dp', 'section')), may hold values from -0.09375 to 0.09375
- start_row: bfloat16 [4096], replicated, may hold values from -6 to 6
- action_table: bfloat16 [256, 4096], replicated, may hold values from -6 to 6
- final_gain: bfloat16 [4096], replicated, may hold values from 0.25 to 1.75
- head_w: bfloat16 [4096, 256], replicated, may hold values from -0.25 to 0.25
Outputs:
- hidden_out: bfloat16 [16, 256, 4096], P(('dp', 'section'), 'tensor')
- loss: float32 [16, 7], P(('dp', 'section'))
The draws below stay inside these ranges and needn't reach their ends.
All inputs are finite; a program needn't handle non-finite values.
Results may differ from the reference program's by a relative error of at most 0.0054.
Values may be sent and summed in bfloat16 or wider, within the bound.
A program may use at most 128 MiB of HBM per device.

```python
import math
import jax
import jax.numpy as jnp
from jax import lax

D = 4096
HEADS = 32
HD = 128
V = 1152
P_SIZE = 256
BINS = 256
ADIM = 7
SLOTS = 8
FRAMES = 16


def touch_ends(values, rng, low, largest):
    place = [jax.random.randint(jax.random.fold_in(rng, axis), (), 0, length) for axis, length in enumerate(values.shape)]
    main_axis = values.shape.index(max(values.shape))
    beside = place[:main_axis] + [(place[main_axis] + 1) % values.shape[main_axis]] + place[main_axis + 1:]
    return values.at[tuple(place)].set(low).at[tuple(beside)].set(largest)


def shard_levels(rng, shape, pieces, smallest, largest):
    def one(axis_at, blocks):
        heights = jax.random.uniform(jax.random.fold_in(jax.random.fold_in(rng, 6), axis_at), (blocks,), jnp.float32, smallest / len(pieces), largest / len(pieces))
        return jnp.repeat(jnp.exp(heights), shape[axis_at] // blocks).reshape((-1,) + (1,) * (len(shape) - axis_at - 1))

    loudness = one(*pieces[0])
    for cut in pieces[1:]:
        loudness = loudness * one(*cut)
    return loudness


def scatter_about(own_key, shape, deviation, reach, cuts=(), kind=jnp.bfloat16):
    array = jax.random.normal(own_key, shape, jnp.float32) * deviation
    if len(cuts) > 0:
        array = shard_levels(own_key, shape, cuts, -0.22, 0.18) * array
    return jnp.clip(array, min=-reach, max=reach).astype(kind)


def setup_inputs(seed: int = 0) -> dict:
    splits = jax.random.split(jax.random.key(seed), 13)
    return {
        "patches": scatter_about(splits[0], (FRAMES, P_SIZE, V), 1.0, 6.0, ((0, 8), (1, 4))),
        "teacher": touch_ends(jax.random.randint(splits[1], (FRAMES, ADIM), 0, BINS), jax.random.fold_in(splits[1], 1), 0, BINS - 1).astype(jnp.int32),
        "proj_w": scatter_about(splits[2], (V, D), V ** -0.5, 0.1875, ((1, 32),)),
        "norm_gain": jnp.clip(1.0 + 0.15 * jax.random.normal(splits[3], (D,), jnp.float32), 0.25, 1.75).astype(jnp.bfloat16),
        "wq": scatter_about(splits[4], (D, D), D ** -0.5, 0.09375, ((0, 8), (1, 4))),
        "wk": scatter_about(splits[5], (D, D), D ** -0.5, 0.09375, ((0, 8), (1, 4))),
        "wv": scatter_about(splits[6], (D, D), D ** -0.5, 0.09375, ((0, 8), (1, 4))),
        "wo": scatter_about(splits[7], (D, D), D ** -0.5, 0.09375, ((0, 4), (1, 8))),
        "start_row": scatter_about(splits[8], (D,), 1.0, 6.0),
        "action_table": scatter_about(splits[9], (BINS, D), 1.0, 6.0),
        "final_gain": jnp.clip(1.0 + 0.15 * jax.random.normal(splits[10], (D,), jnp.float32), 0.25, 1.75).astype(jnp.bfloat16),
        "head_w": scatter_about(splits[11], (D, BINS), (D // 9) ** -0.5, 0.25),
    }


eps = 1e-05

def normalize(rows, gain):
    rows = rows.astype(jnp.float32)
    factor = lax.rsqrt(lax.optimization_barrier(jnp.mean(rows * rows, axis=-1, keepdims=True)) + eps)
    return rows * factor * gain.astype(jnp.float32)

def action_rows(teacher, start_row, action_table):
    frames = teacher.shape[0]
    onehot = (teacher[..., None] == jnp.arange(BINS, dtype=jnp.int32)).astype(jnp.bfloat16)
    looked = jnp.dot(onehot.reshape(-1, BINS), action_table, preferred_element_type=jnp.float32)
    looked = looked.astype(jnp.bfloat16).reshape(frames, ADIM, D)
    start = jnp.broadcast_to(start_row.reshape(1, 1, D), (frames, 1, D))
    return jnp.concatenate([start, looked], axis=1)

def reference(patches, teacher, proj_w, norm_gain, wq, wk, wv, wo, start_row, action_table, final_gain, head_w):
    frames = patches.shape[0]
    length = P_SIZE + SLOTS
    embedded = jnp.dot(patches.reshape(-1, V), proj_w, preferred_element_type=jnp.float32)
    embedded = embedded.astype(jnp.bfloat16).reshape(frames, P_SIZE, D)
    actions = action_rows(teacher, start_row, action_table)
    stream = jnp.concatenate([embedded, actions], axis=1)
    normed = normalize(stream, norm_gain).astype(jnp.bfloat16).reshape(-1, D)
    queries = jnp.dot(normed, wq, preferred_element_type=jnp.float32).astype(jnp.bfloat16).reshape(frames, length, HEADS, HD)
    keys_all = jnp.dot(normed, wk, preferred_element_type=jnp.float32).astype(jnp.bfloat16).reshape(frames, length, HEADS, HD)
    values_all = jnp.dot(normed, wv, preferred_element_type=jnp.float32).astype(jnp.bfloat16).reshape(frames, length, HEADS, HD)
    positions = jnp.arange(length, dtype=jnp.int32)
    causal = positions[:, None] >= positions[None, :]
    inv_root = 1.0 / math.sqrt(HD)

    def one_frame(items):
        query_f, key_f, value_f = items
        scores = jnp.einsum('qhd,khd->hqk', query_f.astype(jnp.float32), key_f.astype(jnp.float32)) * inv_root
        scores = jnp.where(causal[None], scores, -1e+30)
        weights = jax.nn.softmax(scores, axis=-1).astype(jnp.bfloat16)
        result = jnp.einsum('hqk,khd->qhd', weights.astype(jnp.float32), value_f.astype(jnp.float32))
        return result.astype(jnp.bfloat16)
    mixed = lax.map(one_frame, (queries, keys_all, values_all)).reshape(-1, D)
    update = jnp.dot(mixed, wo, preferred_element_type=jnp.float32).reshape(frames, length, D)
    hidden_out = (embedded.astype(jnp.float32) + update[:, :P_SIZE]).astype(jnp.bfloat16)
    acted = actions[:, :ADIM].astype(jnp.float32) + update[:, P_SIZE:P_SIZE + ADIM]
    final = normalize(acted, final_gain).astype(jnp.bfloat16).reshape(-1, D)
    logits = jnp.dot(final, head_w, preferred_element_type=jnp.float32).reshape(frames, ADIM, BINS)
    chosen = (teacher[..., None] == jnp.arange(BINS, dtype=jnp.int32)).astype(jnp.float32)
    picked = lax.optimization_barrier(jnp.sum(logits * chosen, axis=-1))
    loss = jax.nn.logsumexp(logits, axis=-1) - picked
    return (hidden_out, loss)
```

```python
import math

import jax
import jax.numpy as jnp
from jax import lax
from jax.sharding import PartitionSpec as P

D = 4096
HD = 128
V = 1152
P_SIZE = 256
BINS = 256
ADIM = 7
SLOTS = 8


eps = 1e-05


def normalize(rows, gain):
    rows = rows.astype(jnp.float32)
    factor = lax.rsqrt(jnp.mean(rows * rows, axis=-1, keepdims=True) + eps)
    return rows * factor * gain.astype(jnp.float32)


def action_rows(teacher, start_row, action_table):
    frames = teacher.shape[0]
    onehot = (teacher[..., None] == jnp.arange(BINS, dtype=jnp.int32)).astype(jnp.bfloat16)
    looked = jnp.dot(onehot.reshape(-1, BINS), action_table, preferred_element_type=jnp.float32)
    looked = looked.astype(jnp.bfloat16).reshape(frames, ADIM, D)
    start = jnp.broadcast_to(start_row.reshape(1, 1, D), (frames, 1, D))
    return jnp.concatenate([start, looked], axis=1)


def line_gather(own, axis):
    n = lax.axis_size(axis)
    here = lax.axis_index(axis)
    right = left = own
    from_left, from_right = [], []
    for r in range(n - 1):
        right = lax.ppermute(right, axis, [(t, t + 1) for t in range(r, n - 1)])
        left = lax.ppermute(left, axis, [(t, t - 1) for t in range(1, n - r)])
        from_left.append(right)
        from_right.append(left)
    blocks = jnp.zeros((n,) + own.shape, own.dtype)
    blocks = lax.dynamic_update_index_in_dim(blocks, own, here, 0)
    for r in range(n - 1):
        block = jnp.where(here > r, from_left[r], from_right[n - 2 - r])
        blocks = lax.dynamic_update_index_in_dim(blocks, block, lax.rem(here - 1 - r + n, n), 0)
    return blocks


def line_reduce_scatter(parts, axis):
    n = lax.axis_size(axis)
    here = lax.axis_index(axis)

    def part(c):
        return lax.dynamic_index_in_dim(parts, jnp.clip(c, 0, n - 1), 0, keepdims=False)

    right = left = None
    for r in range(n - 1):
        steps = range(min(r, n - 2) + 1)
        to_right = part(n - 1 - r + here)
        to_left = part(r - (n - 1) + here)
        if right is not None:
            to_right = to_right + right.astype(jnp.float32)
            to_left = to_left + left.astype(jnp.float32)
        right = lax.ppermute(to_right.astype(jnp.bfloat16), axis, [(t, t + 1) for t in steps])
        left = lax.ppermute(
            to_left.astype(jnp.bfloat16), axis, [(n - 1 - t, n - 2 - t) for t in steps]
        )
    total = part(here)
    if right is not None:
        total = total + right.astype(jnp.float32) + left.astype(jnp.float32)
    return total


WO_CHUNKS = 2


def on_device(
    patches, teacher, proj_w, norm_gain, wq, wk, wv, wo, start_row, action_table, final_gain, head_w
):
    frames = patches.shape[0]
    local_patches = patches.shape[1]
    length = P_SIZE + SLOTS
    plane = ("dp", "section")
    n_dp, n_t, n_s = (lax.axis_size(a) for a in ("dp", "tensor", "section"))
    here = lax.axis_index("tensor")
    proj_part = lax.all_gather(proj_w, plane, axis=1, tiled=True)
    all_patches = line_gather(patches.reshape(-1, V), "tensor")
    all_patches = all_patches.reshape(n_t, frames, local_patches, V).transpose(1, 0, 2, 3)
    embedded_part = jnp.dot(
        all_patches.reshape(-1, V), proj_part, preferred_element_type=jnp.float32
    ).astype(jnp.bfloat16)
    blocks = line_gather(embedded_part, "tensor")
    embedded_all = (
        blocks.reshape(n_t, frames * P_SIZE, n_dp, -1)
        .transpose(1, 2, 0, 3)
        .reshape(frames, P_SIZE, D)
    )
    embedded_own = lax.dynamic_slice_in_dim(embedded_all, here * local_patches, local_patches, 1)
    actions = action_rows(teacher, start_row, action_table)
    stream = jnp.concatenate([embedded_all, actions], axis=1)
    normed = normalize(stream, norm_gain).astype(jnp.bfloat16).reshape(-1, D)
    local_width = wq.shape[1]
    projected = tuple(
        jnp.dot(
            normed,
            lax.all_gather(weight, plane, axis=0, tiled=True),
            preferred_element_type=jnp.float32,
        )
        for weight in (wq, wk, wv)
    )
    heads_local = local_width // HD
    queries, keys_all, values_all = [
        part.astype(jnp.bfloat16).reshape(frames, length, heads_local, HD) for part in projected
    ]
    inv_root = 1.0 / math.sqrt(HD)
    scores = (
        jnp.einsum("fqhd,fkhd->fhqk", queries, keys_all, preferred_element_type=jnp.float32)
        * inv_root
    )
    positions = jnp.arange(length, dtype=jnp.int32)
    causal = positions[:, None] >= positions[None, :]
    scores = jnp.where(causal[None, None], scores, -1e30)
    weights = jax.nn.softmax(scores, axis=-1).astype(jnp.bfloat16)
    mixed = jnp.einsum("fhqk,fkhd->fqhd", weights, values_all, preferred_element_type=jnp.float32)
    mixed = mixed.astype(jnp.bfloat16).reshape(frames, length, local_width)
    patch_rows = mixed[:, :P_SIZE].reshape(frames, n_t, local_patches, local_width)
    patch_rows = patch_rows.transpose(1, 0, 2, 3).reshape(n_t, -1, local_width)
    slot_rows = mixed[:, P_SIZE:].reshape(n_t, -1, local_width)
    n_patch = frames * local_patches
    ordered = jnp.concatenate([patch_rows, slot_rows], axis=1)
    chunk = wo.shape[1] // WO_CHUNKS
    updates = []
    for j in range(WO_CHUNKS):
        wo_part = lax.all_gather(wo[:, j * chunk : (j + 1) * chunk], plane, axis=1, tiled=True)
        parts = jnp.einsum("nrw,wc->nrc", ordered, wo_part, preferred_element_type=jnp.float32)
        reduced = line_reduce_scatter(parts, "tensor")
        updates.append(reduced.reshape(-1, n_dp * n_s, 1, chunk))
    update = jnp.concatenate(updates, axis=2).reshape(-1, D)
    hidden_out = (
        embedded_own.astype(jnp.float32) + update[:n_patch].reshape(frames, local_patches, D)
    ).astype(jnp.bfloat16)
    own_slots = frames * SLOTS // n_t
    own_actions = lax.dynamic_slice_in_dim(actions.reshape(-1, D), here * own_slots, own_slots, 0)
    acted = own_actions.astype(jnp.float32) + update[n_patch:]
    final = normalize(acted, final_gain).astype(jnp.bfloat16)
    logits = jnp.dot(final, head_w, preferred_element_type=jnp.float32)
    targets = jnp.pad(teacher, ((0, 0), (0, SLOTS - ADIM))).reshape(-1)
    targets = lax.dynamic_slice_in_dim(targets, here * own_slots, own_slots, 0)
    chosen = (targets[:, None] == jnp.arange(BINS, dtype=jnp.int32)).astype(jnp.float32)
    picked = jnp.sum(logits * chosen, axis=-1)
    own_loss = jax.nn.logsumexp(logits, axis=-1) - picked
    loss = lax.all_gather(own_loss, "tensor", axis=0, tiled=True)
    return (hidden_out, loss.reshape(frames, SLOTS)[:, :ADIM])


def solution(mesh):
    return jax.shard_map(
        on_device,
        mesh=mesh,
        in_specs=(
            P(("dp", "section"), "tensor", None),
            P(("dp", "section"), None),
            P(None, ("dp", "tensor", "section")),
            P(),
            P(("dp", "section"), "tensor"),
            P(("dp", "section"), "tensor"),
            P(("dp", "section"), "tensor"),
            P("tensor", ("dp", "section")),
            P(),
            P(),
            P(),
            P(),
        ),
        out_specs=(P(("dp", "section"), "tensor", None), P(("dp", "section"), None)),
        check_vma=False,
    )
```

```python
import math

import jax
import jax.numpy as jnp
from jax import lax
from jax.sharding import PartitionSpec as P

D = 4096
HD = 128
V = 1152
P_SIZE = 256
BINS = 256
ADIM = 7
SLOTS = 8


eps = 1e-05


def normalize(rows, gain):
    rows = rows.astype(jnp.float32)
    factor = lax.rsqrt(jnp.mean(rows * rows, axis=-1, keepdims=True) + eps)
    return rows * factor * gain.astype(jnp.float32)


def action_rows(teacher, start_row, action_table):
    frames = teacher.shape[0]
    onehot = (teacher[..., None] == jnp.arange(BINS, dtype=jnp.int32)).astype(jnp.bfloat16)
    looked = jnp.dot(onehot.reshape(-1, BINS), action_table, preferred_element_type=jnp.float32)
    looked = looked.astype(jnp.bfloat16).reshape(frames, ADIM, D)
    start = jnp.broadcast_to(start_row.reshape(1, 1, D), (frames, 1, D))
    return jnp.concatenate([start, looked], axis=1)


def line_gather(own, axis):
    n = lax.axis_size(axis)
    here = lax.axis_index(axis)
    right = left = own
    from_left, from_right = [], []
    for r in range(n - 1):
        right = lax.ppermute(right, axis, [(t, t + 1) for t in range(r, n - 1)])
        left = lax.ppermute(left, axis, [(t, t - 1) for t in range(1, n - r)])
        from_left.append(right)
        from_right.append(left)
    blocks = jnp.zeros((n,) + own.shape, own.dtype)
    blocks = lax.dynamic_update_index_in_dim(blocks, own, here, 0)
    for r in range(n - 1):
        block = jnp.where(here > r, from_left[r], from_right[n - 2 - r])
        blocks = lax.dynamic_update_index_in_dim(blocks, block, lax.rem(here - 1 - r + n, n), 0)
    return blocks


def line_reduce_scatter(parts, axis):
    n = lax.axis_size(axis)
    here = lax.axis_index(axis)

    def part(c):
        return lax.dynamic_index_in_dim(parts, jnp.clip(c, 0, n - 1), 0, keepdims=False)

    right = left = None
    for r in range(n - 1):
        steps = range(min(r, n - 2) + 1)
        to_right = part(n - 1 - r + here)
        to_left = part(r - (n - 1) + here)
        if right is not None:
            to_right = to_right + right.astype(jnp.float32)
            to_left = to_left + left.astype(jnp.float32)
        right = lax.ppermute(to_right.astype(jnp.bfloat16), axis, [(t, t + 1) for t in steps])
        left = lax.ppermute(
            to_left.astype(jnp.bfloat16), axis, [(n - 1 - t, n - 2 - t) for t in steps]
        )
    total = part(here)
    if right is not None:
        total = total + right.astype(jnp.float32) + left.astype(jnp.float32)
    return total


def plane_columns(own):
    rows, columns = own.shape
    blocks = line_gather(line_gather(own, "section").reshape(-1, columns), "dp")
    blocks = blocks.reshape(-1, rows, columns)
    return jnp.concatenate([blocks[i] for i in range(blocks.shape[0])], axis=1)


RELAYS = 2


def on_device(
    patches, teacher, proj_w, norm_gain, wq, wk, wv, wo, start_row, action_table, final_gain, head_w
):
    frames = patches.shape[0]
    local_patches = patches.shape[1]
    length = P_SIZE + SLOTS
    plane = ("dp", "section")
    n_dp, n_t = lax.axis_size("dp"), lax.axis_size("tensor")
    here = lax.axis_index("tensor")
    proj_part = plane_columns(proj_w)
    all_patches = line_gather(patches.reshape(-1, V), "tensor")
    all_patches = all_patches.reshape(n_t, frames, local_patches, V).transpose(1, 0, 2, 3)
    embedded_part = jnp.dot(
        all_patches.reshape(-1, V), proj_part, preferred_element_type=jnp.float32
    ).astype(jnp.bfloat16)
    blocks = line_gather(embedded_part, "tensor")
    width = embedded_part.shape[1] // n_dp
    embedded_all = jnp.concatenate(
        [blocks[t, :, d * width : (d + 1) * width] for d in range(n_dp) for t in range(n_t)], axis=1
    ).reshape(frames, P_SIZE, D)
    embedded_own = lax.dynamic_slice_in_dim(embedded_all, here * local_patches, local_patches, 1)
    actions = action_rows(teacher, start_row, action_table)
    stream = jnp.concatenate([embedded_all, actions], axis=1)
    normed = normalize(stream, norm_gain).astype(jnp.bfloat16).reshape(-1, D)
    full_out = plane_columns(wo)
    local_width = wq.shape[1]
    projected = tuple(
        jnp.dot(
            normed,
            lax.all_gather(weight, plane, axis=0, tiled=True),
            preferred_element_type=jnp.float32,
        )
        for weight in (wq, wk, wv)
    )
    heads_local = local_width // HD
    queries, keys_all, values_all = [
        part.astype(jnp.bfloat16).reshape(frames, length, heads_local, HD) for part in projected
    ]
    inv_root = 1.0 / math.sqrt(HD)
    scores = (
        jnp.einsum("fqhd,fkhd->fhqk", queries, keys_all, preferred_element_type=jnp.float32)
        * inv_root
    )
    positions = jnp.arange(length, dtype=jnp.int32)
    causal = positions[:, None] >= positions[None, :]
    scores = jnp.where(causal[None, None], scores, -1e30)
    weights = jax.nn.softmax(scores, axis=-1).astype(jnp.bfloat16)
    mixed = jnp.einsum("fhqk,fkhd->fqhd", weights, values_all, preferred_element_type=jnp.float32)
    mixed = mixed.astype(jnp.bfloat16).reshape(frames, length, local_width)
    patch_rows = mixed[:, :P_SIZE].reshape(frames, n_t, local_patches, local_width)
    patch_rows = patch_rows.transpose(1, 0, 2, 3).reshape(n_t, -1, local_width)
    slot_rows = mixed[:, P_SIZE:].reshape(-1, local_width)
    slot_part = jnp.dot(slot_rows, full_out, preferred_element_type=jnp.float32)
    slot_parts = line_gather(slot_part.astype(jnp.bfloat16), "tensor")
    slot_update = jnp.sum(slot_parts.astype(jnp.float32), axis=0)
    chunk = D // RELAYS
    updates = []
    for j in range(RELAYS):
        parts = jnp.einsum(
            "nrw,wc->nrc",
            patch_rows,
            full_out[:, j * chunk : (j + 1) * chunk],
            preferred_element_type=jnp.float32,
        )
        updates.append(line_reduce_scatter(parts, "tensor"))
    update = jnp.concatenate(updates, axis=1).reshape(frames, local_patches, D)
    hidden_out = (embedded_own.astype(jnp.float32) + update).astype(jnp.bfloat16)
    acted = (actions.astype(jnp.float32) + slot_update.reshape(frames, SLOTS, D))[:, :ADIM]
    final = normalize(acted, final_gain).astype(jnp.bfloat16).reshape(-1, D)
    logits = jnp.dot(final, head_w, preferred_element_type=jnp.float32).reshape(frames, ADIM, BINS)
    chosen = (teacher[..., None] == jnp.arange(BINS, dtype=jnp.int32)).astype(jnp.float32)
    picked = jnp.sum(logits * chosen, axis=-1)
    loss = jax.nn.logsumexp(logits, axis=-1) - picked
    return (hidden_out, loss)


def solution(mesh):
    return jax.shard_map(
        on_device,
        mesh=mesh,
        in_specs=(
            P(("dp", "section"), "tensor", None),
            P(("dp", "section"), None),
            P(None, ("dp", "tensor", "section")),
            P(),
            P(("dp", "section"), "tensor"),
            P(("dp", "section"), "tensor"),
            P(("dp", "section"), "tensor"),
            P("tensor", ("dp", "section")),
            P(),
            P(),
            P(),
            P(),
        ),
        out_specs=(P(("dp", "section"), "tensor", None), P(("dp", "section"), None)),
        check_vma=False,
    )
```
